32 devices in a mesh: groups: 2 (over y), pts: 4 (over z), cb: 4 (over x, core).
Axes of the slice: x: 2, y: 2, z: 4, core: 2. Of those that a mesh axis runs over, the one named last changes fastest.
Arguments:
- points: bfloat16 [16384, 768], P(('groups', 'pts')), parts along dimension 0, may hold values from -60 to 60
- code_one: int32 [16384], P(('groups', 'pts')), parts along dimension 0, may hold values from 0 to 2047
- code_two: int32 [16384], P(('groups', 'pts')), parts along dimension 0, may hold values from 0 to 2047
- cent_one: bfloat16 [4096, 768], P(('groups', 'cb')), parts along dimension 0, may hold values from -6 to 6
- cent_two: bfloat16 [4096, 768], P(('groups', 'cb')), parts along dimension 0, may hold values from -6 to 6
Outputs:
- new_one: bfloat16 [4096, 768], P(('groups', 'cb')), parts along dimension 0
- new_two: bfloat16 [4096, 768], P(('groups', 'cb')), parts along dimension 0
- distortion: float32 [4], P('groups'), parts along dimension 0
The draws below stay inside these ranges and needn't reach their ends.
There are 2 independent parts, one for each index of `groups`. The reference program is written for one: setup_inputs(seed, part) draws one part's arguments, and reference() takes and returns one part's arrays. A program takes and returns all parts, laid end to end along the dimension named above; each array names one. Nothing has to cross between parts.
All inputs are finite; a program needn't handle non-finite values.
Results may differ from the reference program's by a relative error of at most 0.0014.
Values may be sent and summed in bfloat16 or wider, within the bound.
A program may use at most 64 MiB of HBM per device.

```python
import math
import jax
import jax.numpy as jnp
from jax import lax

D = 768
K = 2048
POINTS = 8192


def centre_table(key):
    values = jax.random.normal(jax.random.fold_in(key, 11), (K, D), jnp.float32)
    return jnp.clip(values, -6.0, 6.0).astype(jnp.bfloat16)


def draw_cent_one(key, part):
    return centre_table(key)


def draw_points(key, part):
    centres = centre_table(key).astype(jnp.float32)
    picks = jax.random.randint(jax.random.fold_in(key, 12), (POINTS,), 0, K)
    chosen = jnp.take(centres, picks, axis=0)
    key_jit = jax.random.fold_in(jax.random.fold_in(key, 13), 0)
    key_base = jax.random.fold_in(jax.random.fold_in(key, 13), 1)
    key_cols = jax.random.fold_in(jax.random.fold_in(key, 13), 3)
    rowpos = jnp.arange(POINTS, dtype=jnp.float32) / POINTS
    trend = jnp.power(3.0, rowpos)
    jitter = jnp.exp(jax.random.uniform(key_jit, (POINTS,), jnp.float32, 0.0, math.log(4.0)))
    colscale = jnp.exp(jax.random.uniform(key_cols, (D,), jnp.float32, math.log(0.5), math.log(2.0)))
    base = jax.random.normal(key_base, (POINTS, D), jnp.float32)
    noise = 0.15 * base * (trend * jitter)[:, None] * colscale[None, :]
    return jnp.clip(chosen + noise, -60.0, 60.0).astype(jnp.bfloat16)


def plant(result, own_key, smallest, high):
    shape = result.shape
    place = [jax.random.randint(jax.random.fold_in(own_key, axis), (), 0, shape[axis]) for axis in range(len(shape))]
    result = result.at[tuple(place)].set(smallest)
    longest = shape.index(max(shape))
    place[longest] = (place[longest] + 1) % shape[longest]
    return result.at[tuple(place)].set(high)


def levels(stream_key, shape, cuts, smallest, top_value):
    def one(axis_at, parts):
        steps = jax.random.uniform(jax.random.fold_in(jax.random.fold_in(stream_key, 6), axis_at), (parts,), jnp.float32, smallest / len(cuts), top_value / len(cuts))
        return jnp.repeat(jnp.exp(steps), shape[axis_at] // parts).reshape((-1,) + (1,) * (len(shape) - axis_at - 1))

    level = one(*cuts[0])
    for cut in cuts[1:]:
        level = level * one(*cut)
    return level


def normal_values(key, dims, scale, limit, cuts=(), kind=jnp.bfloat16):
    level = levels(key, dims, cuts, -0.22, 0.18) if cuts else 1.0
    result = jax.random.normal(key, dims, jnp.float32) * scale * level
    return jnp.minimum(jnp.maximum(result, -limit), limit).astype(kind)


def setup_inputs(seed: int = 0, part: int = 0) -> dict:
    keys = jax.random.split(jax.random.key(seed), 6)
    part_keys = jax.random.split(jax.random.fold_in(keys[5], part), 6)
    return {
        "points": draw_points(jax.random.fold_in(jax.random.fold_in(keys[5], part), 71), part),
        "code_one": plant(jax.random.randint(part_keys[1], (POINTS,), 0, K), jax.random.fold_in(part_keys[1], 1), 0, K - 1).astype(jnp.int32),
        "code_two": plant(jax.random.randint(part_keys[2], (POINTS,), 0, K), jax.random.fold_in(part_keys[2], 1), 0, K - 1).astype(jnp.int32),
        "cent_one": draw_cent_one(jax.random.fold_in(jax.random.fold_in(keys[5], part), 71), part),
        "cent_two": normal_values(part_keys[4], (K, D), 1.0, 6.0, ((0, 4),)),
    }


def nearest_total(data, cents):
    csq = jnp.sum(jnp.square(cents.astype(jnp.float32)), axis=1)
    block = math.gcd(POINTS, 4096)
    blocks = data.reshape(POINTS // block, block, D)

    def one_block(rows_in):
        sq = jnp.sum(jnp.square(rows_in.astype(jnp.float32)), axis=1)
        cross = lax.dot_general(rows_in, cents, (((1,), (1,)), ((), ())), preferred_element_type=jnp.float32)
        dist = sq[:, None] - 2.0 * cross + csq[None, :]
        return jnp.min(dist, axis=1)

    mins = lax.map(one_block, blocks)
    return jnp.sum(mins)


def update(data, codes, cents):
    sums = jax.ops.segment_sum(data.astype(jnp.float32), codes, num_segments=K)
    counts = jax.ops.segment_sum(jnp.ones((POINTS,), jnp.float32), codes, num_segments=K)
    return ((sums + cents.astype(jnp.float32)) / (counts + 1.0)[:, None]).astype(jnp.bfloat16)


def reference(points, code_one, code_two, cent_one, cent_two):
    new_one = update(points, code_one, cent_one)
    looked = jnp.take(new_one, code_one, axis=0)
    residual = (points.astype(jnp.float32) - looked.astype(jnp.float32)).astype(jnp.bfloat16)
    new_two = update(residual, code_two, cent_two)
    first = nearest_total(points, cent_one)
    second = nearest_total(residual, cent_two)
    distortion = jnp.stack([first, second]) / jnp.float32(POINTS * D)
    return new_one, new_two, distortion
```

```python
import functools

import jax
import jax.numpy as jnp
from jax import lax
from jax.experimental import pallas as pl
from jax.experimental.pallas import tpu as pltpu
from jax.sharding import PartitionSpec as P

F32 = jnp.float32
BF16 = jnp.bfloat16
CORES = 2


def fused_kernel(
    npts, ncb,
    points, code_one, code_two, cent_one, cent_two,
    new_one, new_two, total_out,
    residual, codebook, sums, from_left, from_right, codes_all, mins, mins_in, tot, tot_in,
    rs_send, rs_left, rs_right, ag_send, ag_left, ag_right,
    x_send, x_recv, d_send, d_recv, code_send, code_recv, min_send, min_recv, tot_send, tot_recv,
):
    p = lax.axis_index("pts")
    c = lax.axis_index("cb")
    npoints, width = points.shape
    rows = cent_one.shape[0]
    share = rows // npts
    ids = rows * ncb
    nx = ncb // CORES
    cx, cc = c // CORES, c % CORES
    sibling = cx * CORES + (1 - cc)

    def to_pts(src, dst, s, r, where):
        return pltpu.make_async_remote_copy(
            src_ref=src, dst_ref=dst, send_sem=s, recv_sem=r,
            device_id={"pts": where}, device_id_type=pl.DeviceIdType.MESH,
        )

    def to_cb(src, dst, s, r, where):
        return pltpu.make_async_remote_copy(
            src_ref=src, dst_ref=dst, send_sem=s, recv_sem=r,
            device_id={"cb": where}, device_id_type=pl.DeviceIdType.MESH,
        )

    barrier = pltpu.get_barrier_semaphore()
    for d in range(1, npts):
        pl.semaphore_signal(barrier, inc=1, device_id={"pts": (p + d) % npts},
                            device_id_type=pl.DeviceIdType.MESH)
    for d in range(1, ncb):
        pl.semaphore_signal(barrier, inc=1, device_id={"cb": (c + d) % ncb},
                            device_id_type=pl.DeviceIdType.MESH)

    def partial_sums(data, code):
        def one(t, carry):
            label = c * rows + t * share + lax.broadcasted_iota(jnp.int32, (share, npoints), 0)
            onehot = jnp.where(code[...] == label, 1.0, 0.0).astype(BF16)
            sums[t] = jnp.dot(onehot, data[...], preferred_element_type=F32)
            return carry

        lax.fori_loop(0, npts, one, 0)

    def send_right(k, t):
        return to_pts(sums.at[t], from_left.at[k, t], rs_send.at[k, t], rs_left.at[k, t], p + 1)

    def send_left(k, t):
        return to_pts(sums.at[t], from_right.at[k, t], rs_send.at[k, t], rs_right.at[k, t], p - 1)

    def reduce_first(k):
        @pl.when(p == 0)
        def _():
            for s in range(npts - 1):
                send_right(k, npts - 1 - s).start()

        @pl.when(p == npts - 1)
        def _():
            for s in range(npts - 1):
                send_left(k, s).start()

    def reduce_rest(k):
        inner = jnp.logical_and(p > 0, p < npts - 1)
        for s in range(npts - 1):
            t_right, t_left = npts - 1 - s, s

            @pl.when(jnp.logical_and(inner, p < t_right))
            def _():
                send_right(k, t_right).wait_recv()
                sums[t_right] += from_left[k, t_right]
                send_right(k, t_right).start()

            @pl.when(jnp.logical_and(inner, p > t_left))
            def _():
                send_left(k, t_left).wait_recv()
                sums[t_left] += from_right[k, t_left]
                send_left(k, t_left).start()

    def reduce_last(k):
        @pl.when(p > 0)
        def _():
            send_right(k, p).wait_recv()
            sums[p] += from_left[k, p]

        @pl.when(p < npts - 1)
        def _():
            send_left(k, p).wait_recv()
            sums[p] += from_right[k, p]

    def reduce_sent(k):
        for t in range(npts):
            @pl.when(p < t)
            def _():
                send_right(k, t).wait_send()

            @pl.when(p > t)
            def _():
                send_left(k, t).wait_send()

    def counts(k):
        label = c * rows + p * share + lax.broadcasted_iota(jnp.int32, (share, npoints), 0)

        def one(t, acc):
            return acc + jnp.where(codes_all[k, t] == label, 1.0, 0.0)

        acc = lax.fori_loop(0, npts, one, jnp.zeros((share, npoints), F32))
        return jnp.sum(acc, axis=1, keepdims=True)

    def finish(k, cents, count, out, at):
        old = cents[pl.ds(pl.multiple_of(p * share, share), share), :].astype(F32)
        out[pl.ds(at, share), :] = ((sums[p] + old) / (count + 1.0)).astype(BF16)

    def nearest(k, data, cents):
        step = npoints // 8
        cent = cents[...]
        csq = jnp.sum(jnp.square(cent.astype(F32)), axis=1, keepdims=True)
        scaled = cent * (-2.0)

        def one(i, acc):
            at = pl.ds(pl.multiple_of(i * step, step), step)
            block = data[at, :]
            cross = lax.dot_general(scaled.astype(BF16), block, (((1,), (1,)), ((), ())),
                                    preferred_element_type=F32)
            mins[k, :, at] = jnp.min(cross + csq, axis=0, keepdims=True)
            sq = jnp.square(block.astype(F32))
            return acc + jnp.sum(sq.reshape(step // 8, 8, width), axis=0)

        acc = lax.fori_loop(0, 8, one, jnp.zeros((8, width), F32))
        return jnp.sum(acc, keepdims=True)

    def row_block(col, t):
        return pl.ds(pl.multiple_of(col * rows + t * share, share), share)

    partial_sums(points, code_one)
    pl.semaphore_wait(barrier, npts - 1 + ncb - 1)
    reduce_first(0)
    for k, code in enumerate((code_one, code_two)):
        for d in range(1, npts):
            to_pts(code, codes_all.at[k, p], code_send.at[k, d], code_recv.at[k, d],
                   (p + d) % npts).start()
        codes_all[k, p] = code[...]
    sq_one = nearest(0, points, cent_one)
    for k, code in enumerate((code_one, code_two)):
        for d in range(1, npts):
            to_pts(code, codes_all.at[k, (p + npts - d) % npts], code_send.at[k, d],
                   code_recv.at[k, d], (p + d) % npts).wait()
    count_one = counts(0)
    reduce_rest(0)
    count_two = counts(1)
    reduce_last(0)
    reduce_sent(0)
    finish(0, cent_one, count_one, codebook, pl.multiple_of(c * rows + p * share, share))

    def ag_right_copy(t):
        block = codebook.at[row_block(c, t), :]
        return to_pts(block, block, ag_send.at[0, t], ag_left.at[t], p + 1)

    def ag_left_copy(t):
        block = codebook.at[row_block(c, t), :]
        return to_pts(block, block, ag_send.at[1, t], ag_right.at[t], p - 1)

    def x_copy(o, t, col):
        block = codebook.at[row_block(col, t), :]
        return to_cb(block, block, x_send.at[o, t], x_recv.at[o, t], ((cx + o) % nx) * CORES + cc)

    def d_copy(o, t, col):
        block = codebook.at[row_block(col, t), :]
        return to_cb(block, block, d_send.at[o, t], d_recv.at[o, t], sibling)

    def spread(t):
        for o in range(1, nx):
            x_copy(o, t, c).start()
        d_copy(0, t, c).start()

    def gather_own(do_spread, right_copy, left_copy):
        for s in range(npts):
            for way in ((0,) if s == 0 else (0, 1)):
                t = p - s if way == 0 else p + s

                @pl.when(jnp.logical_and(t >= 0, t < npts))
                def _():
                    if s > 0 and way == 0:
                        right_copy(t).wait_recv()
                    if s > 0 and way == 1:
                        left_copy(t).wait_recv()
                    if way == 0:
                        @pl.when(p < npts - 1)
                        def _():
                            right_copy(t).start()
                    if way == 1 or s == 0:
                        @pl.when(p > 0)
                        def _():
                            left_copy(t).start()
                    if do_spread:
                        spread(t)

    def gather_own_sent(right_copy, left_copy):
        for t in range(npts):
            @pl.when(jnp.logical_and(t <= p, p < npts - 1))
            def _():
                right_copy(t).wait_send()

            @pl.when(jnp.logical_and(t >= p, p > 0))
            def _():
                left_copy(t).wait_send()

    gather_own(True, ag_right_copy, ag_left_copy)
    for s in range(npts):
        for way in ((0,) if s == 0 else (0, 1)):
            t = p - s if way == 0 else p + s

            @pl.when(jnp.logical_and(t >= 0, t < npts))
            def _():
                for o in range(1, nx):
                    src = ((cx + nx - o) % nx) * CORES + cc
                    x_copy(o, t, src).wait_recv()
                    d_copy(o, t, src).start()
    for t in range(npts):
        for o in range(nx):
            d_copy(o, t, ((cx + nx - o) % nx) * CORES + 1 - cc).wait_recv()
    for t in range(npts):
        for o in range(nx):
            d_copy(o, t, ((cx + nx - o) % nx) * CORES + cc).wait_send()
            if o > 0:
                x_copy(o, t, c).wait_send()
    gather_own_sent(ag_right_copy, ag_left_copy)
    new_one[...] = codebook[pl.ds(pl.multiple_of(c * rows, rows), rows), :]

    tile = 128
    group = 4

    def look(i, carry):
        blocks = []
        for j in range(group):
            at = pl.ds(pl.multiple_of((i * group + j) * tile, tile), tile)
            blocks.append(jnp.broadcast_to(code_one[:, at], (tile, tile)).T)
        column = jnp.concatenate(blocks, axis=0)
        wide = jnp.concatenate([column] * (ids // tile), axis=1)
        label = lax.broadcasted_iota(jnp.int32, (group * tile, ids), 1)
        onehot = jnp.where(wide == label, 1.0, 0.0).astype(BF16)
        looked = jnp.dot(onehot, codebook[...], preferred_element_type=F32)
        at = pl.ds(pl.multiple_of(i * group * tile, group * tile), group * tile)
        residual[at, :] = (points[at, :].astype(F32) - looked).astype(BF16)
        return carry

    lax.fori_loop(0, npoints // (group * tile), look, 0)

    partial_sums(residual, code_two)
    reduce_first(1)
    sq_two = nearest(1, residual, cent_two)
    for d in range(1, ncb):
        to_cb(mins, mins_in.at[d], min_send.at[d], min_recv.at[d], (c + d) % ncb).start()
    reduce_rest(1)
    for d in range(1, ncb):
        to_cb(mins, mins_in.at[d], min_send.at[d], min_recv.at[d], (c + d) % ncb).wait()
    best = mins[...]
    for d in range(1, ncb):
        best = jnp.minimum(best, mins_in[d])
    for k, sq in enumerate((sq_one, sq_two)):
        tot[k] = jnp.broadcast_to(jnp.sum(best[k], keepdims=True) + sq, tot.shape[1:])
    for d in range(1, npts):
        to_pts(tot, tot_in.at[d], tot_send.at[d], tot_recv.at[d], (p + d) % npts).start()
    reduce_last(1)
    reduce_sent(1)
    finish(1, cent_two, count_two, new_two, pl.multiple_of(p * share, share))

    def two_right_copy(t):
        block = new_two.at[pl.ds(pl.multiple_of(t * share, share), share), :]
        return to_pts(block, block, ag_send.at[2, t], ag_left.at[npts + t], p + 1)

    def two_left_copy(t):
        block = new_two.at[pl.ds(pl.multiple_of(t * share, share), share), :]
        return to_pts(block, block, ag_send.at[3, t], ag_right.at[npts + t], p - 1)

    gather_own(False, two_right_copy, two_left_copy)
    for d in range(1, npts):
        to_pts(tot, tot_in.at[d], tot_send.at[d], tot_recv.at[d], (p + d) % npts).wait()
    total = tot[...]
    for d in range(1, npts):
        total = total + tot_in[d]
    total_out[...] = total / F32(npoints * npts * width)
    gather_own_sent(two_right_copy, two_left_copy)


def fused(points, code_one, code_two, cent_one, cent_two):
    npts = lax.axis_size("pts")
    ncb = lax.axis_size("cb")
    npoints, width = points.shape
    rows = cent_one.shape[0]
    share = rows // npts
    nx = ncb // CORES
    vmem = pl.BlockSpec(memory_space=pltpu.VMEM)
    dma = pltpu.SemaphoreType.DMA
    new_one, new_two, total = pl.pallas_call(
        functools.partial(fused_kernel, npts, ncb),
        out_shape=(
            jax.ShapeDtypeStruct(cent_one.shape, BF16),
            jax.ShapeDtypeStruct(cent_two.shape, BF16),
            jax.ShapeDtypeStruct((2, 1, 128), F32),
        ),
        in_specs=[vmem] * 5,
        out_specs=(vmem,) * 3,
        scratch_shapes=[
            pltpu.VMEM(points.shape, BF16),
            pltpu.VMEM((rows * ncb, width), BF16),
            pltpu.VMEM((npts, share, width), F32),
            pltpu.VMEM((2, npts, share, width), F32),
            pltpu.VMEM((2, npts, share, width), F32),
            pltpu.VMEM((2, npts, 1, npoints), jnp.int32),
            pltpu.VMEM((2, 1, npoints), F32),
            pltpu.VMEM((ncb, 2, 1, npoints), F32),
            pltpu.VMEM((2, 1, 128), F32),
            pltpu.VMEM((npts, 2, 1, 128), F32),
            dma((2, npts)), dma((2, npts)), dma((2, npts)),
            dma((4, npts)), dma((2 * npts,)), dma((2 * npts,)),
            dma((nx, npts)), dma((nx, npts)), dma((nx, npts)), dma((nx, npts)),
            dma((2, npts)), dma((2, npts)), dma((ncb,)), dma((ncb,)), dma((npts,)), dma((npts,)),
        ],
        compiler_params=pltpu.CompilerParams(
            collective_id=0, has_side_effects=True, vmem_limit_bytes=60 * 1024 * 1024
        ),
    )(points, code_one.reshape(1, npoints), code_two.reshape(1, npoints), cent_one, cent_two)
    return new_one, new_two, total[:, 0, 0]


def nearest_local(data, cents):
    sq = jnp.sum(jnp.square(data.astype(jnp.float32)), axis=1)
    csq = jnp.sum(jnp.square(cents.astype(jnp.float32)), axis=1)
    cross = lax.dot_general(
        data, cents, (((1,), (1,)), ((), ())), preferred_element_type=jnp.float32
    )
    dist = sq[:, None] - 2.0 * cross + csq[None, :]
    local_min = jnp.min(dist, axis=1)
    best = lax.pmin(local_min, "cb")
    return jnp.sum(best)


def section_update(data, codes, cents):
    rows = cents.shape[0]
    first = lax.axis_index("cb") * rows
    labels = first + lax.broadcasted_iota(jnp.int32, (1, rows), 1)
    onehot = (codes[:, None] == labels).astype(jnp.bfloat16)
    sums = lax.dot_general(
        onehot, data, (((0,), (0,)), ((), ())), preferred_element_type=jnp.float32
    )
    counts = jnp.sum(onehot.astype(jnp.float32), axis=0)
    share_sums, share_counts = (
        lax.psum_scatter(sums, "pts", scatter_dimension=0, tiled=True),
        lax.psum_scatter(counts, "pts", scatter_dimension=0, tiled=True),
    )
    share_rows = share_sums.shape[0]
    old_rows = lax.dynamic_slice_in_dim(cents, lax.axis_index("pts") * share_rows, share_rows, 0)
    return ((share_sums + old_rows.astype(jnp.float32)) / (share_counts + 1.0)[:, None]).astype(
        jnp.bfloat16
    )


def section_total(value):
    return lax.psum(value, "pts")


def local(points, code_one, code_two, cent_one, cent_two):
    rows = cent_one.shape[0]
    width = points.shape[1]
    npts = lax.axis_size("pts")
    ncb = lax.axis_size("cb")
    first = lax.axis_index("cb") * rows
    first_local = nearest_local(points, cent_one)
    updated_one = section_update(points, code_one, cent_one)
    gathered = lax.all_gather(updated_one, ("pts", "cb"), axis=0, tiled=True)
    share_rows = updated_one.shape[0]
    codebook = jnp.swapaxes(gathered.reshape(npts, ncb, share_rows, width), 0, 1).reshape(
        rows * ncb, width
    )
    new_one = lax.dynamic_slice_in_dim(codebook, first, rows, 0)
    looked = jnp.take(codebook, code_one, axis=0)
    residual = (points.astype(jnp.float32) - looked.astype(jnp.float32)).astype(jnp.bfloat16)
    updated_two = section_update(residual, code_two, cent_two)
    new_two = lax.all_gather(updated_two, "pts", axis=0, tiled=True)
    second_local = nearest_local(residual, cent_two)
    first_sum = section_total(first_local)
    second_sum = section_total(second_local)
    scale = jnp.float32(points.shape[0] * npts * width)
    distortion = jnp.stack([first_sum, second_sum]) / scale
    return (new_one, new_two, distortion)


def choose(points, code_one, code_two, cent_one, cent_two):
    rows, npts, ncb = cent_one.shape[0], lax.axis_size("pts"), lax.axis_size("cb")
    fits = rows % (16 * npts) == 0 and ncb % CORES == 0 and points.shape[0] % 1024 == 0
    form = fused if fits else local
    return form(points, code_one, code_two, cent_one, cent_two)


def solution(mesh):
    return jax.shard_map(
        choose,
        mesh=mesh,
        in_specs=(
            P(("groups", "pts"), None),
            P(("groups", "pts")),
            P(("groups", "pts")),
            P(("groups", "cb"), None),
            P(("groups", "cb"), None),
        ),
        out_specs=(P(("groups", "cb"), None), P(("groups", "cb"), None), P("groups")),
        check_vma=False,
    )
```

```python
import functools

import jax
import jax.numpy as jnp
from jax import lax
from jax.experimental import pallas as pl
from jax.experimental.pallas import tpu as pltpu
from jax.sharding import PartitionSpec as P

F32 = jnp.float32
BF16 = jnp.bfloat16
CORES = 2
PARTS = 8
LAG = 2
WINDOW = 2


def fused_kernel(
    npts, ncb, parts, lag, window,
    points, code_one, code_two, cent_one, cent_two,
    new_one, new_two, total_out,
    residual, codebook, sums, from_left, from_right, codes_all, mins, mins_in, tot, tot_in,
    scaled, csq, squares,
    rs_send, rs_recv, ag_send, ag_recv,
    x_send, x_recv, d_send, d_recv, code_send, code_recv, min_send, min_recv, tot_send, tot_recv,
):
    p = lax.axis_index("pts")
    c = lax.axis_index("cb")
    last = npts - 1
    npoints, width = points.shape
    rows = cent_one.shape[0]
    size = rows // (2 * parts)
    ids = rows * ncb
    nx = ncb // CORES
    cx, cc = c // CORES, c % CORES
    sibling = cx * CORES + (1 - cc)

    def to(axis, src, dst, s, r, where):
        return pltpu.make_async_remote_copy(
            src_ref=src, dst_ref=dst, send_sem=s, recv_sem=r,
            device_id={axis: where}, device_id_type=pl.DeviceIdType.MESH,
        )

    barrier = pltpu.get_barrier_semaphore()
    for d in range(1, npts):
        pl.semaphore_signal(barrier, inc=1, device_id={"pts": (p + d) % npts},
                            device_id_type=pl.DeviceIdType.MESH)
    for d in range(1, ncb):
        pl.semaphore_signal(barrier, inc=1, device_id={"cb": (c + d) % ncb},
                            device_id_type=pl.DeviceIdType.MESH)

    span = rows // npts

    def partial_sums(data, code):
        def one(t, carry):
            label = c * rows + t * span + lax.broadcasted_iota(jnp.int32, (span, npoints), 0)
            onehot = jnp.where(code[...] == label, 1.0, 0.0).astype(BF16)
            at = pl.ds(pl.multiple_of(t * span, span), span)
            sums[at, :] = jnp.dot(onehot, data[...], preferred_element_type=F32)
            return carry

        lax.fori_loop(0, npts, one, 0)

    def code_copy(k, d, slot):
        code = (code_one, code_two)[k]
        return to("pts", code, codes_all.at[k, slot], code_send.at[k, d], code_recv.at[k, d],
                  (p + d) % npts)

    def part(g):
        return pl.ds(pl.multiple_of(g * size, size), size)

    def count(k, g):
        label = c * rows + g * size + lax.broadcasted_iota(jnp.int32, (size, npoints), 0)
        acc = jnp.zeros((size, npoints), F32)
        for t in range(npts):
            acc = acc + jnp.where(codes_all[k, t] == label, 1.0, 0.0)
        return jnp.sum(acc, axis=1, keepdims=True)

    pieces = 8
    step = npoints // pieces

    def near_start(cents):
        cent = cents[...]
        csq[...] = jnp.sum(jnp.square(cent.astype(F32)), axis=1, keepdims=True)
        scaled[...] = (cent * (-2.0)).astype(BF16)
        squares[...] = jnp.zeros(squares.shape, F32)

    def near_piece(k, data, i):
        at = pl.ds(pl.multiple_of(i * step, step), step)
        block = data[at, :]
        cross = lax.dot_general(scaled[...], block, (((1,), (1,)), ((), ())),
                                preferred_element_type=F32)
        mins[k, :, at] = jnp.min(cross + csq[...], axis=0, keepdims=True)
        sq = jnp.square(block.astype(F32))
        squares[...] += jnp.sum(sq.reshape(step // 8, 8, width), axis=0)

    def exchange(k, data, cents, table, base, share_out):
        def row(g):
            return table.at[pl.ds(pl.multiple_of(base + g * size, size), size), :]

        def rs(way, j):
            g = j + (parts if way == 1 else 0)
            land = from_left if way == 1 else from_right
            return to("pts", sums.at[part(g), :], land.at[k, j], rs_send.at[k, way, j],
                      rs_recv.at[k, way, j], p + 1 if way == 1 else p - 1)

        def ag(way, j):
            g = j + (parts if way == 1 else 0)
            return to("pts", row(g), row(g), ag_send.at[k, way, j], ag_recv.at[k, way, j],
                      p - 1 if way == 1 else p + 1)

        def block(col, g):
            at = pl.multiple_of(col * rows + g * size, size)
            return codebook.at[pl.ds(at, size), :]

        def x_copy(o, g):
            return to("cb", block(c, g), block(c, g), x_send.at[o, g], x_recv.at[o, g],
                      ((cx + o) % nx) * CORES + cc)

        def d_copy(o, g):
            ref = block(((cx + nx - o) % nx) * CORES + cc, g)
            return to("cb", ref, ref, d_send.at[o, g], d_recv.at[o, g], sibling)

        def spread(g):
            if share_out:
                for o in range(1, nx):
                    x_copy(o, g).start()
                d_copy(0, g).start()

        def run(i, carry):
            for way in (1, 0):
                first, end = (0, last) if way == 1 else (last, 0)
                shift = parts if way == 1 else 0
                near_end = p if way == 1 else last - p
                j = i - lag * near_end

                @pl.when(jnp.logical_and(j >= 0, j < parts))
                def _():
                    @pl.when(p != first)
                    def _():
                        rs(way, j).wait_recv()
                        land = from_left if way == 1 else from_right
                        sums[part(j + shift), :] += land[k, j]

                    @pl.when(p != end)
                    def _():
                        @pl.when(j >= window)
                        def _():
                            rs(way, j - window).wait_send()

                        rs(way, j).start()

                    @pl.when(p == end)
                    def _():
                        g = j + shift
                        old = cents[part(g), :].astype(F32)
                        row(g)[...] = (
                            (sums[part(g), :] + old) / (count(k, g) + 1.0)
                        ).astype(BF16)
                        ag(way, j).start()
                        spread(g)

                back = i - lag * (2 * last) + lag * near_end

                @pl.when(jnp.logical_and(p != end, jnp.logical_and(back >= 0, back < parts)))
                def _():
                    ag(way, back).wait_recv()

                    @pl.when(p != first)
                    def _():
                        ag(way, back).start()

                    spread(back + shift)

                if share_out:
                    over = back - lag

                    @pl.when(jnp.logical_and(over >= 0, over < parts))
                    def _():
                        for o in range(1, nx):
                            x_copy(o, over + shift).wait_recv()
                            d_copy(o, over + shift).start()

            @pl.when(i < pieces)
            def _():
                near_piece(k, data, i)

            if k == 0:
                @pl.when(i == lag)
                def _():
                    for kk in range(2):
                        for d in range(1, npts):
                            code_copy(kk, d, (p + npts - d) % npts).wait()
            else:
                @pl.when(i == pieces)
                def _():
                    for d in range(1, ncb):
                        min_copy(d).start()

                @pl.when(i == pieces + 2 * lag)
                def _():
                    totals()

            return carry

        steps = parts + 2 * lag * last + (lag if share_out else 0)
        lax.fori_loop(0, max(steps, pieces + 2 * lag + 1), run, 0)

        def drain(j, carry):
            for way in (1, 0):
                first, end = (0, last) if way == 1 else (last, 0)
                shift = parts if way == 1 else 0

                @pl.when(jnp.logical_and(p != end, j >= parts - window))
                def _():
                    rs(way, j).wait_send()

                @pl.when(p != first)
                def _():
                    ag(way, j).wait_send()

                if share_out:
                    for o in range(nx):
                        d_copy(o, j + shift).wait()
                        if o > 0:
                            x_copy(o, j + shift).wait_send()
            return carry

        lax.fori_loop(0, parts, drain, 0)

    def min_copy(d):
        return to("cb", mins, mins_in.at[d], min_send.at[d], min_recv.at[d], (c + d) % ncb)

    def tot_copy(d):
        return to("pts", tot, tot_in.at[d], tot_send.at[d], tot_recv.at[d], (p + d) % npts)

    def totals():
        for d in range(1, ncb):
            min_copy(d).wait()
        best = mins[...]
        for d in range(1, ncb):
            best = jnp.minimum(best, mins_in[d])
        squares_two = jnp.sum(squares[...], keepdims=True)
        for k in range(2):
            sq = squares_two if k == 1 else tot[0, :, :1]
            tot[k] = jnp.broadcast_to(jnp.sum(best[k], keepdims=True) + sq, tot.shape[1:])
        for d in range(1, npts):
            tot_copy(d).start()

    partial_sums(points, code_one)
    near_start(cent_one)
    pl.semaphore_wait(barrier, npts - 1 + ncb - 1)
    for k, code in enumerate((code_one, code_two)):
        for d in range(1, npts):
            code_copy(k, d, p).start()
        codes_all[k, p] = code[...]
    exchange(0, points, cent_one, codebook, c * rows, True)
    tot[0] = jnp.broadcast_to(jnp.sum(squares[...], keepdims=True), tot.shape[1:])

    tile = 128
    group = 4

    def look(i, carry):
        blocks = []
        for j in range(group):
            at = pl.ds(pl.multiple_of((i * group + j) * tile, tile), tile)
            blocks.append(jnp.broadcast_to(code_one[:, at], (tile, tile)).T)
        column = jnp.concatenate(blocks, axis=0)
        wide = jnp.concatenate([column] * (ids // tile), axis=1)
        label = lax.broadcasted_iota(jnp.int32, (group * tile, ids), 1)
        onehot = jnp.where(wide == label, 1.0, 0.0).astype(BF16)
        looked = jnp.dot(onehot, codebook[...], preferred_element_type=F32)
        at = pl.ds(pl.multiple_of(i * group * tile, group * tile), group * tile)
        residual[at, :] = (points[at, :].astype(F32) - looked).astype(BF16)
        return carry

    lax.fori_loop(0, npoints // (group * tile), look, 0)
    partial_sums(residual, code_two)
    near_start(cent_two)
    exchange(1, residual, cent_two, new_two, 0, False)
    new_one[...] = codebook[pl.ds(pl.multiple_of(c * rows, rows), rows), :]
    for d in range(1, npts):
        tot_copy(d).wait()
    total = tot[...]
    for d in range(1, npts):
        total = total + tot_in[d]
    total_out[...] = total / F32(npoints * npts * width)


def fused(points, code_one, code_two, cent_one, cent_two):
    npts = lax.axis_size("pts")
    ncb = lax.axis_size("cb")
    npoints, width = points.shape
    rows = cent_one.shape[0]
    nx = ncb // CORES
    parts = PARTS
    size = rows // (2 * parts)
    vmem = pl.BlockSpec(memory_space=pltpu.VMEM)
    dma = pltpu.SemaphoreType.DMA
    new_one, new_two, total = pl.pallas_call(
        functools.partial(fused_kernel, npts, ncb, parts, LAG, WINDOW),
        out_shape=(
            jax.ShapeDtypeStruct(cent_one.shape, BF16),
            jax.ShapeDtypeStruct(cent_two.shape, BF16),
            jax.ShapeDtypeStruct((2, 1, 128), F32),
        ),
        in_specs=[vmem] * 5,
        out_specs=(vmem,) * 3,
        scratch_shapes=[
            pltpu.VMEM(points.shape, BF16),
            pltpu.VMEM((rows * ncb, width), BF16),
            pltpu.VMEM((rows, width), F32),
            pltpu.VMEM((2, parts, size, width), F32),
            pltpu.VMEM((2, parts, size, width), F32),
            pltpu.VMEM((2, npts, 1, npoints), jnp.int32),
            pltpu.VMEM((2, 1, npoints), F32),
            pltpu.VMEM((ncb, 2, 1, npoints), F32),
            pltpu.VMEM((2, 1, 128), F32),
            pltpu.VMEM((npts, 2, 1, 128), F32),
            pltpu.VMEM((rows, width), BF16),
            pltpu.VMEM((rows, 1), F32),
            pltpu.VMEM((8, width), F32),
            dma((2, 2, parts)), dma((2, 2, parts)), dma((2, 2, parts)), dma((2, 2, parts)),
            dma((nx, 2 * parts)), dma((nx, 2 * parts)), dma((nx, 2 * parts)),
            dma((nx, 2 * parts)),
            dma((2, npts)), dma((2, npts)), dma((ncb,)), dma((ncb,)), dma((npts,)), dma((npts,)),
        ],
        compiler_params=pltpu.CompilerParams(
            collective_id=0, has_side_effects=True, vmem_limit_bytes=60 * 1024 * 1024
        ),
    )(points, code_one.reshape(1, npoints), code_two.reshape(1, npoints), cent_one, cent_two)
    return new_one, new_two, total[:, 0, 0]


def nearest_local(data, cents):
    sq = jnp.sum(jnp.square(data.astype(jnp.float32)), axis=1)
    csq = jnp.sum(jnp.square(cents.astype(jnp.float32)), axis=1)
    cross = lax.dot_general(
        data, cents, (((1,), (1,)), ((), ())), preferred_element_type=jnp.float32
    )
    dist = sq[:, None] - 2.0 * cross + csq[None, :]
    local_min = jnp.min(dist, axis=1)
    best = lax.pmin(local_min, "cb")
    return jnp.sum(best)


def section_update(data, codes, cents):
    rows = cents.shape[0]
    first = lax.axis_index("cb") * rows
    labels = first + lax.broadcasted_iota(jnp.int32, (1, rows), 1)
    onehot = (codes[:, None] == labels).astype(jnp.bfloat16)
    sums = lax.dot_general(
        onehot, data, (((0,), (0,)), ((), ())), preferred_element_type=jnp.float32
    )
    counts = jnp.sum(onehot.astype(jnp.float32), axis=0)
    share_sums, share_counts = (
        lax.psum_scatter(sums, "pts", scatter_dimension=0, tiled=True),
        lax.psum_scatter(counts, "pts", scatter_dimension=0, tiled=True),
    )
    share_rows = share_sums.shape[0]
    old_rows = lax.dynamic_slice_in_dim(cents, lax.axis_index("pts") * share_rows, share_rows, 0)
    return ((share_sums + old_rows.astype(jnp.float32)) / (share_counts + 1.0)[:, None]).astype(
        jnp.bfloat16
    )


def section_total(value):
    return lax.psum(value, "pts")


def local(points, code_one, code_two, cent_one, cent_two):
    rows = cent_one.shape[0]
    width = points.shape[1]
    npts = lax.axis_size("pts")
    ncb = lax.axis_size("cb")
    first = lax.axis_index("cb") * rows
    first_local = nearest_local(points, cent_one)
    updated_one = section_update(points, code_one, cent_one)
    gathered = lax.all_gather(updated_one, ("pts", "cb"), axis=0, tiled=True)
    share_rows = updated_one.shape[0]
    codebook = jnp.swapaxes(gathered.reshape(npts, ncb, share_rows, width), 0, 1).reshape(
        rows * ncb, width
    )
    new_one = lax.dynamic_slice_in_dim(codebook, first, rows, 0)
    looked = jnp.take(codebook, code_one, axis=0)
    residual = (points.astype(jnp.float32) - looked.astype(jnp.float32)).astype(jnp.bfloat16)
    updated_two = section_update(residual, code_two, cent_two)
    new_two = lax.all_gather(updated_two, "pts", axis=0, tiled=True)
    second_local = nearest_local(residual, cent_two)
    first_sum = section_total(first_local)
    second_sum = section_total(second_local)
    scale = jnp.float32(points.shape[0] * npts * width)
    distortion = jnp.stack([first_sum, second_sum]) / scale
    return (new_one, new_two, distortion)


def choose(points, code_one, code_two, cent_one, cent_two):
    rows, npts, ncb = cent_one.shape[0], lax.axis_size("pts"), lax.axis_size("cb")
    fits = (
        1 < npts <= 8
        and rows % (32 * PARTS) == 0
        and rows % (16 * npts) == 0
        and ncb % CORES == 0
        and points.shape[0] % 1024 == 0
    )
    form = fused if fits else local
    return form(points, code_one, code_two, cent_one, cent_two)


def solution(mesh):
    return jax.shard_map(
        choose,
        mesh=mesh,
        in_specs=(
            P(("groups", "pts"), None),
            P(("groups", "pts")),
            P(("groups", "pts")),
            P(("groups", "cb"), None),
            P(("groups", "cb"), None),
        ),
        out_specs=(P(("groups", "cb"), None), P(("groups", "cb"), None), P("groups")),
        check_vma=False,
    )
```

```python
import functools

import jax
import jax.numpy as jnp
from jax import lax
from jax.experimental import pallas as pl
from jax.experimental.pallas import tpu as pltpu
from jax.sharding import PartitionSpec as P

F32 = jnp.float32
BF16 = jnp.bfloat16
CORES = 2
PARTS = 8
LAG = 3
WINDOW = 2


def fused_kernel(
    npts, ncb, parts, lag, window,
    points, code_one, code_two, cent_one, cent_two,
    new_one, new_two, total_out,
    residual, codebook, sums, from_left, from_right, codes_all, mins, mins_in, tot, tot_in,
    scaled, csq, squares,
    rs_send, rs_recv, ag_send, ag_recv,
    x_send, x_recv, d_send, d_recv, code_send, code_recv, min_send, min_recv, tot_send, tot_recv,
):
    p = lax.axis_index("pts")
    c = lax.axis_index("cb")
    last = npts - 1
    npoints, width = points.shape
    rows = cent_one.shape[0]
    size = rows // (2 * parts)
    ids = rows * ncb
    nx = ncb // CORES
    cx, cc = c // CORES, c % CORES
    sibling = cx * CORES + (1 - cc)

    def to(axis, src, dst, s, r, where):
        return pltpu.make_async_remote_copy(
            src_ref=src, dst_ref=dst, send_sem=s, recv_sem=r,
            device_id={axis: where}, device_id_type=pl.DeviceIdType.MESH,
        )

    barrier = pltpu.get_barrier_semaphore()
    for d in range(1, npts):
        pl.semaphore_signal(barrier, inc=1, device_id={"pts": (p + d) % npts},
                            device_id_type=pl.DeviceIdType.MESH)
    for d in range(1, ncb):
        pl.semaphore_signal(barrier, inc=1, device_id={"cb": (c + d) % ncb},
                            device_id_type=pl.DeviceIdType.MESH)

    span = rows // npts

    def partial_sums(data, code):
        def one(t, carry):
            label = c * rows + t * span + lax.broadcasted_iota(jnp.int32, (span, npoints), 0)
            onehot = jnp.where(code[...] == label, 1.0, 0.0).astype(BF16)
            at = pl.ds(pl.multiple_of(t * span, span), span)
            sums[at, :] = jnp.dot(onehot, data[...], preferred_element_type=F32)
            return carry

        lax.fori_loop(0, npts, one, 0)

    def code_copy(k, d, slot):
        code = (code_one, code_two)[k]
        return to("pts", code, codes_all.at[k, slot], code_send.at[k, d], code_recv.at[k, d],
                  (p + d) % npts)

    def part(g):
        return pl.ds(pl.multiple_of(g * size, size), size)

    def count(k, g):
        label = c * rows + g * size + lax.broadcasted_iota(jnp.int32, (size, npoints), 0)
        acc = jnp.zeros((size, npoints), F32)
        for t in range(npts):
            acc = acc + jnp.where(codes_all[k, t] == label, 1.0, 0.0)
        return jnp.sum(acc, axis=1, keepdims=True)

    pieces = 8
    step = npoints // pieces

    def near_start(cents):
        cent = cents[...]
        csq[...] = jnp.sum(jnp.square(cent.astype(F32)), axis=1, keepdims=True)
        scaled[...] = (cent * (-2.0)).astype(BF16)
        squares[...] = jnp.zeros(squares.shape, F32)

    def near_piece(k, data, i):
        at = pl.ds(pl.multiple_of(i * step, step), step)
        block = data[at, :]
        cross = lax.dot_general(scaled[...], block, (((1,), (1,)), ((), ())),
                                preferred_element_type=F32)
        mins[k, :, at] = jnp.min(cross + csq[...], axis=0, keepdims=True)
        sq = jnp.square(block.astype(F32))
        squares[...] += jnp.sum(sq.reshape(step // 8, 8, width), axis=0)

    def exchange(k, data, cents, table, base, share_out):
        def row(g):
            return table.at[pl.ds(pl.multiple_of(base + g * size, size), size), :]

        def rs(way, j):
            g = j + (parts if way == 1 else 0)
            land = from_left if way == 1 else from_right
            return to("pts", sums.at[part(g), :], land.at[k, j], rs_send.at[k, way, j],
                      rs_recv.at[k, way, j], p + 1 if way == 1 else p - 1)

        def ag(way, j):
            g = j + (parts if way == 1 else 0)
            return to("pts", row(g), row(g), ag_send.at[k, way, j], ag_recv.at[k, way, j],
                      p - 1 if way == 1 else p + 1)

        def block(col, g):
            at = pl.multiple_of(col * rows + g * size, size)
            return codebook.at[pl.ds(at, size), :]

        def x_copy(o, g):
            return to("cb", block(c, g), block(c, g), x_send.at[o, g], x_recv.at[o, g],
                      ((cx + o) % nx) * CORES + cc)

        def d_copy(o, g):
            ref = block(((cx + nx - o) % nx) * CORES + cc, g)
            return to("cb", ref, ref, d_send.at[o, g], d_recv.at[o, g], sibling)

        def spread(g):
            if share_out:
                for o in range(1, nx):
                    x_copy(o, g).start()
                d_copy(0, g).start()

        def run(i, carry):
            for way in (1, 0):
                first, end = (0, last) if way == 1 else (last, 0)
                shift = parts if way == 1 else 0
                near_end = p if way == 1 else last - p
                j = i - lag * near_end

                @pl.when(jnp.logical_and(j >= 0, j < parts))
                def _():
                    @pl.when(p != first)
                    def _():
                        rs(way, j).wait_recv()
                        land = from_left if way == 1 else from_right
                        sums[part(j + shift), :] += land[k, j]

                    @pl.when(p != end)
                    def _():
                        @pl.when(j >= window)
                        def _():
                            rs(way, j - window).wait_send()

                        rs(way, j).start()

                    @pl.when(p == end)
                    def _():
                        g = j + shift
                        old = cents[part(g), :].astype(F32)
                        row(g)[...] = (
                            (sums[part(g), :] + old) / (count(k, g) + 1.0)
                        ).astype(BF16)
                        ag(way, j).start()
                        spread(g)

                back = i - lag * (2 * last) + lag * near_end

                @pl.when(jnp.logical_and(p != end, jnp.logical_and(back >= 0, back < parts)))
                def _():
                    ag(way, back).wait_recv()

                    @pl.when(p != first)
                    def _():
                        ag(way, back).start()

                    spread(back + shift)

                if share_out:
                    over = back - lag

                    @pl.when(jnp.logical_and(over >= 0, over < parts))
                    def _():
                        for o in range(1, nx):
                            x_copy(o, over + shift).wait_recv()
                            d_copy(o, over + shift).start()

            @pl.when(i < pieces)
            def _():
                near_piece(k, data, i)

            if k == 0:
                @pl.when(i == lag)
                def _():
                    for kk in range(2):
                        for d in range(1, npts):
                            code_copy(kk, d, (p + npts - d) % npts).wait()
            else:
                @pl.when(i == pieces)
                def _():
                    for d in range(1, ncb):
                        min_copy(d).start()

                @pl.when(i == pieces + 2 * lag)
                def _():
                    totals()

            return carry

        steps = parts + 2 * lag * last + (lag if share_out else 0)
        lax.fori_loop(0, max(steps, pieces + 2 * lag + 1), run, 0)

        def drain(j, carry):
            for way in (1, 0):
                first, end = (0, last) if way == 1 else (last, 0)
                shift = parts if way == 1 else 0

                @pl.when(jnp.logical_and(p != end, j >= parts - window))
                def _():
                    rs(way, j).wait_send()

                @pl.when(p != first)
                def _():
                    ag(way, j).wait_send()

                if share_out:
                    for o in range(nx):
                        d_copy(o, j + shift).wait()
                        if o > 0:
                            x_copy(o, j + shift).wait_send()
            return carry

        lax.fori_loop(0, parts, drain, 0)

    def min_copy(d):
        return to("cb", mins, mins_in.at[d], min_send.at[d], min_recv.at[d], (c + d) % ncb)

    def tot_copy(d):
        return to("pts", tot, tot_in.at[d], tot_send.at[d], tot_recv.at[d], (p + d) % npts)

    def totals():
        for d in range(1, ncb):
            min_copy(d).wait()
        best = mins[...]
        for d in range(1, ncb):
            best = jnp.minimum(best, mins_in[d])
        squares_two = jnp.sum(squares[...], keepdims=True)
        for k in range(2):
            sq = squares_two if k == 1 else tot[0, :, :1]
            tot[k] = jnp.broadcast_to(jnp.sum(best[k], keepdims=True) + sq, tot.shape[1:])
        for d in range(1, npts):
            tot_copy(d).start()

    partial_sums(points, code_one)
    near_start(cent_one)
    pl.semaphore_wait(barrier, npts - 1 + ncb - 1)
    for k, code in enumerate((code_one, code_two)):
        for d in range(1, npts):
            code_copy(k, d, p).start()
        codes_all[k, p] = code[...]
    exchange(0, points, cent_one, codebook, c * rows, True)
    tot[0] = jnp.broadcast_to(jnp.sum(squares[...], keepdims=True), tot.shape[1:])

    tile = 128
    group = 4

    def look(i, carry):
        blocks = []
        for j in range(group):
            at = pl.ds(pl.multiple_of((i * group + j) * tile, tile), tile)
            blocks.append(jnp.broadcast_to(code_one[:, at], (tile, tile)).T)
        column = jnp.concatenate(blocks, axis=0)
        wide = jnp.concatenate([column] * (ids // tile), axis=1)
        label = lax.broadcasted_iota(jnp.int32, (group * tile, ids), 1)
        onehot = jnp.where(wide == label, 1.0, 0.0).astype(BF16)
        looked = jnp.dot(onehot, codebook[...], preferred_element_type=F32)
        at = pl.ds(pl.multiple_of(i * group * tile, group * tile), group * tile)
        residual[at, :] = (points[at, :].astype(F32) - looked).astype(BF16)
        return carry

    lax.fori_loop(0, npoints // (group * tile), look, 0)
    partial_sums(residual, code_two)
    near_start(cent_two)
    exchange(1, residual, cent_two, new_two, 0, False)
    new_one[...] = codebook[pl.ds(pl.multiple_of(c * rows, rows), rows), :]
    for d in range(1, npts):
        tot_copy(d).wait()
    total = tot[...]
    for d in range(1, npts):
        total = total + tot_in[d]
    total_out[...] = total / F32(npoints * npts * width)


def fused(points, code_one, code_two, cent_one, cent_two):
    npts = lax.axis_size("pts")
    ncb = lax.axis_size("cb")
    npoints, width = points.shape
    rows = cent_one.shape[0]
    nx = ncb // CORES
    parts = PARTS
    size = rows // (2 * parts)
    vmem = pl.BlockSpec(memory_space=pltpu.VMEM)
    dma = pltpu.SemaphoreType.DMA
    new_one, new_two, total = pl.pallas_call(
        functools.partial(fused_kernel, npts, ncb, parts, LAG, WINDOW),
        out_shape=(
            jax.ShapeDtypeStruct(cent_one.shape, BF16),
            jax.ShapeDtypeStruct(cent_two.shape, BF16),
            jax.ShapeDtypeStruct((2, 1, 128), F32),
        ),
        in_specs=[vmem] * 5,
        out_specs=(vmem,) * 3,
        scratch_shapes=[
            pltpu.VMEM(points.shape, BF16),
            pltpu.VMEM((rows * ncb, width), BF16),
            pltpu.VMEM((rows, width), F32),
            pltpu.VMEM((2, parts, size, width), F32),
            pltpu.VMEM((2, parts, size, width), F32),
            pltpu.VMEM((2, npts, 1, npoints), jnp.int32),
            pltpu.VMEM((2, 1, npoints), F32),
            pltpu.VMEM((ncb, 2, 1, npoints), F32),
            pltpu.VMEM((2, 1, 128), F32),
            pltpu.VMEM((npts, 2, 1, 128), F32),
            pltpu.VMEM((rows, width), BF16),
            pltpu.VMEM((rows, 1), F32),
            pltpu.VMEM((8, width), F32),
            dma((2, 2, parts)), dma((2, 2, parts)), dma((2, 2, parts)), dma((2, 2, parts)),
            dma((nx, 2 * parts)), dma((nx, 2 * parts)), dma((nx, 2 * parts)),
            dma((nx, 2 * parts)),
            dma((2, npts)), dma((2, npts)), dma((ncb,)), dma((ncb,)), dma((npts,)), dma((npts,)),
        ],
        compiler_params=pltpu.CompilerParams(
            collective_id=0, has_side_effects=True, vmem_limit_bytes=60 * 1024 * 1024
        ),
    )(points, code_one.reshape(1, npoints), code_two.reshape(1, npoints), cent_one, cent_two)
    return new_one, new_two, total[:, 0, 0]


def nearest_local(data, cents):
    sq = jnp.sum(jnp.square(data.astype(jnp.float32)), axis=1)
    csq = jnp.sum(jnp.square(cents.astype(jnp.float32)), axis=1)
    cross = lax.dot_general(
        data, cents, (((1,), (1,)), ((), ())), preferred_element_type=jnp.float32
    )
    dist = sq[:, None] - 2.0 * cross + csq[None, :]
    local_min = jnp.min(dist, axis=1)
    best = lax.pmin(local_min, "cb")
    return jnp.sum(best)


def section_update(data, codes, cents):
    rows = cents.shape[0]
    first = lax.axis_index("cb") * rows
    labels = first + lax.broadcasted_iota(jnp.int32, (1, rows), 1)
    onehot = (codes[:, None] == labels).astype(jnp.bfloat16)
    sums = lax.dot_general(
        onehot, data, (((0,), (0,)), ((), ())), preferred_element_type=jnp.float32
    )
    counts = jnp.sum(onehot.astype(jnp.float32), axis=0)
    share_sums, share_counts = (
        lax.psum_scatter(sums, "pts", scatter_dimension=0, tiled=True),
        lax.psum_scatter(counts, "pts", scatter_dimension=0, tiled=True),
    )
    share_rows = share_sums.shape[0]
    old_rows = lax.dynamic_slice_in_dim(cents, lax.axis_index("pts") * share_rows, share_rows, 0)
    return ((share_sums + old_rows.astype(jnp.float32)) / (share_counts + 1.0)[:, None]).astype(
        jnp.bfloat16
    )


def section_total(value):
    return lax.psum(value, "pts")


def local(points, code_one, code_two, cent_one, cent_two):
    rows = cent_one.shape[0]
    width = points.shape[1]
    npts = lax.axis_size("pts")
    ncb = lax.axis_size("cb")
    first = lax.axis_index("cb") * rows
    first_local = nearest_local(points, cent_one)
    updated_one = section_update(points, code_one, cent_one)
    gathered = lax.all_gather(updated_one, ("pts", "cb"), axis=0, tiled=True)
    share_rows = updated_one.shape[0]
    codebook = jnp.swapaxes(gathered.reshape(npts, ncb, share_rows, width), 0, 1).reshape(
        rows * ncb, width
    )
    new_one = lax.dynamic_slice_in_dim(codebook, first, rows, 0)
    looked = jnp.take(codebook, code_one, axis=0)
    residual = (points.astype(jnp.float32) - looked.astype(jnp.float32)).astype(jnp.bfloat16)
    updated_two = section_update(residual, code_two, cent_two)
    new_two = lax.all_gather(updated_two, "pts", axis=0, tiled=True)
    second_local = nearest_local(residual, cent_two)
    first_sum = section_total(first_local)
    second_sum = section_total(second_local)
    scale = jnp.float32(points.shape[0] * npts * width)
    distortion = jnp.stack([first_sum, second_sum]) / scale
    return (new_one, new_two, distortion)


def choose(points, code_one, code_two, cent_one, cent_two):
    rows, npts, ncb = cent_one.shape[0], lax.axis_size("pts"), lax.axis_size("cb")
    fits = (
        1 < npts <= 8
        and rows % (32 * PARTS) == 0
        and rows % (16 * npts) == 0
        and ncb % CORES == 0
        and points.shape[0] % 1024 == 0
    )
    form = fused if fits else local
    return form(points, code_one, code_two, cent_one, cent_two)


def solution(mesh):
    return jax.shard_map(
        choose,
        mesh=mesh,
        in_specs=(
            P(("groups", "pts"), None),
            P(("groups", "pts")),
            P(("groups", "pts")),
            P(("groups", "cb"), None),
            P(("groups", "cb"), None),
        ),
        out_specs=(P(("groups", "cb"), None), P(("groups", "cb"), None), P("groups")),
        check_vma=False,
    )
```
